32 devices in a mesh: gx: 4 (over z), gy: 2 (over core), ta: 4 (over y, x).
Axes of the slice: x: 2, y: 2, z: 4, core: 2. Of those that a mesh axis runs over, the one named last changes fastest.
Arguments:
- links: float32 [4, 2, 3, 3, 8, 4, 4, 128], P(None, None, None, None, 'gx', 'gy', 'ta'), may hold values from -1 to 1, as said below
Outputs:
- flowed: float32 [4, 2, 3, 3, 8, 4, 4, 128], P(None, None, None, None, 'gx', 'gy', 'ta')
- action_slices: float32 [4], P('ta')
The draws below stay inside these ranges and needn't reach their ends.
Inputs may be any that keep to these rules, and one draw needn't show every extreme that they name: `links`: every link is a special unitary 3x3 matrix.
All inputs are finite; a program needn't handle non-finite values.
Results may differ from the reference program's by a relative error of at most 0.0003.
Values sent between devices are 32-bit elements; how exact they have to be, the bound alone decides.
A program may use at most 64 MiB of HBM per device.

```python
import jax
import jax.numpy as jnp
from jax import lax

NZ = 128
NX = 8
NY = 4
NT = 4


def complex_times(former, latter):
    return jnp.stack([former[0] * latter[0] - former[1] * latter[1], former[0] * latter[1] + former[1] * latter[0]])


def normalized(vector):
    length = jnp.sqrt(jnp.sum(vector[0] ** 2 + vector[1] ** 2, axis=0))
    return vector / length


def draw_links(key, part):
    raw = jax.random.normal(key, (2, 3, 3, 4, NX, NY, NT, NZ), jnp.float32)
    row_zero = normalized(raw[:, 0])
    second = raw[:, 1]
    inner_real = jnp.sum(row_zero[0] * second[0] + row_zero[1] * second[1], axis=0)
    inner_imag = jnp.sum(row_zero[0] * second[1] - row_zero[1] * second[0], axis=0)
    projection = jnp.stack([inner_real * row_zero[0] - inner_imag * row_zero[1], inner_real * row_zero[1] + inner_imag * row_zero[0]])
    row_one = normalized(second - projection)
    pieces = []
    for first_col, second_col in ((1, 2), (2, 0), (0, 1)):
        cross = complex_times(row_zero[:, first_col], row_one[:, second_col]) - complex_times(row_zero[:, second_col], row_one[:, first_col])
        pieces.append(jnp.stack([cross[0], -cross[1]]))
    row_two = jnp.stack(pieces, axis=1)
    matrix = jnp.stack([row_zero, row_one, row_two], axis=1)
    return jnp.moveaxis(matrix, 3, 0)


def setup_inputs(seed: int = 0) -> dict:
    key_list = jax.random.split(jax.random.key(seed), 2)
    links = draw_links(jax.random.fold_in(key_list[1], 71), 0)
    return {"links": links}


flow_eps = 0.1
taylor_order = 6


def contract(first_part, second_part):
    return jnp.sum(first_part[:, :, None] * second_part[None, :, :], axis=1)


def matmul_pair(former, latter):
    return jnp.stack([contract(former[0], latter[0]) - contract(former[1], latter[1]),
                      contract(former[0], latter[1]) + contract(former[1], latter[0])])


def adjoint(matrix):
    return jnp.stack([jnp.swapaxes(matrix[0], 0, 1), -jnp.swapaxes(matrix[1], 0, 1)])


def trace_real(former, latter):
    return jnp.sum(former[0] * jnp.swapaxes(latter[0], 0, 1) - former[1] * jnp.swapaxes(latter[1], 0, 1), axis=(0, 1))


def unit_offset(dir_index, sign):
    return tuple(sign if k == dir_index else 0 for k in range(4))


def add_offsets(first_off, second_off):
    return tuple(first_off[k] + second_off[k] for k in range(4))


def shifted(component, offset):
    x_len = component.shape[-4] - 2
    y_len = component.shape[-3] - 2
    t_len = component.shape[-2] - 2
    view = component[..., 1 + offset[0]:1 + offset[0] + x_len, 1 + offset[1]:1 + offset[1] + y_len,
                     1 + offset[2]:1 + offset[2] + t_len, :]
    if offset[3] != 0:
        view = jnp.roll(view, -offset[3], axis=-1)
    return view


def upper_staple(padded, mu_dir, nu_dir):
    here = (0, 0, 0, 0)
    first_pair = matmul_pair(shifted(padded[nu_dir], unit_offset(mu_dir, 1)),
                             adjoint(shifted(padded[mu_dir], unit_offset(nu_dir, 1))))
    return matmul_pair(first_pair, adjoint(shifted(padded[nu_dir], here)))


def lower_corner(padded, mu_dir, nu_dir):
    back = unit_offset(nu_dir, -1)
    corner = add_offsets(unit_offset(mu_dir, 1), back)
    first_pair = matmul_pair(adjoint(shifted(padded[nu_dir], corner)), adjoint(shifted(padded[mu_dir], back)))
    return matmul_pair(first_pair, shifted(padded[nu_dir], back))


def antihermitian(matrix):
    real_part = (matrix[0] - jnp.swapaxes(matrix[0], 0, 1)) / 2.0
    imag_part = (matrix[1] + jnp.swapaxes(matrix[1], 0, 1)) / 2.0
    trace_imag = jnp.trace(matrix[1], axis1=0, axis2=1) / 3.0
    eye = jnp.eye(3, dtype=jnp.float32).reshape((3, 3) + (1,) * (matrix.ndim - 3))
    return jnp.stack([real_part, imag_part - eye * trace_imag])


def flow_force(padded, lower_fn):
    centre = padded[..., 1:-1, 1:-1, 1:-1, :]
    forces = []
    action = jnp.zeros((centre.shape[6],), jnp.float32)
    for mu_dir in range(4):
        link_here = centre[mu_dir]
        staple_sum = jnp.zeros_like(link_here)
        for nu_dir in range(4):
            if nu_dir == mu_dir:
                continue
            upper = upper_staple(padded, mu_dir, nu_dir)
            action = action + jnp.sum(1.0 - trace_real(link_here, upper) / 3.0, axis=(0, 1, 3))
            staple_sum = staple_sum + upper + lower_fn(mu_dir, nu_dir)
        omega = matmul_pair(link_here, staple_sum)
        forces.append(-flow_eps * antihermitian(omega))
    return jnp.stack(forces), action / 2.0


def polynomial_exp(generator):
    eye = jnp.eye(3, dtype=jnp.float32).reshape((3, 3) + (1,) * (generator.ndim - 3))
    identity = jnp.stack([jnp.broadcast_to(eye, generator.shape[1:]), jnp.zeros(generator.shape[1:], jnp.float32)])
    result = identity
    for order in range(taylor_order, 0, -1):
        result = identity + matmul_pair(generator, result) / order
    return result


def advance(generator, links_now):
    def one_direction(gen_dir, link_dir):
        return matmul_pair(polynomial_exp(gen_dir), link_dir)
    return jax.vmap(one_direction)(generator, links_now)


def section_force(links_now):
    extended = jnp.concatenate([links_now[..., -1:, :], links_now, links_now[..., :1, :]], axis=6)

    def slice_force(t_index):
        block = lax.dynamic_slice_in_dim(extended, t_index, 3, axis=6)
        padded = jnp.concatenate([block[..., -1:, :, :, :], block, block[..., :1, :, :, :]], axis=4)
        padded = jnp.concatenate([padded[..., -1:, :, :], padded, padded[..., :1, :, :]], axis=5)

        def lower_fn(mu_dir, nu_dir):
            return lower_corner(padded, mu_dir, nu_dir)
        return flow_force(padded, lower_fn)

    forces, action = lax.map(slice_force, jnp.arange(NT, dtype=jnp.int32))
    forces = jnp.moveaxis(forces[..., 0, :], 0, 6)
    return forces, action.reshape((NT,))


def reference(links):
    force_zero, action = section_force(links)
    section_one = advance(force_zero / 4.0, links)
    force_one, unused_one = section_force(section_one)
    section_two = advance(8.0 / 9.0 * force_one - 17.0 / 36.0 * force_zero, section_one)
    force_two, unused_two = section_force(section_two)
    flowed = advance(3.0 / 4.0 * force_two - 8.0 / 9.0 * force_one + 17.0 / 36.0 * force_zero, section_two)
    action_slices = action / (6.0 * NX * NY * NZ)
    return flowed, action_slices
```

```python
import functools

import jax
import jax.numpy as jnp
from jax import lax
from jax.experimental import pallas as pl
from jax.experimental.pallas import tpu as pltpu
from jax.sharding import PartitionSpec as P

MESH = pl.DeviceIdType.MESH
AXES = ("gx", "gy", "ta")
flow_eps = 0.1
FRESH = (1.0 / 4.0, 8.0 / 9.0, 3.0 / 4.0)
KEPT = (0.0, -17.0 / 9.0, -1.0)


def mul(a, b):
    def dot(x, y):
        return sum(x[:, k][:, None] * y[k][None] for k in range(3))

    return dot(a[0], b[0]) - dot(a[1], b[1]), dot(a[0], b[1]) + dot(a[1], b[0])


def mul_right_adjoint(a, b):
    def dot(x, y):
        return sum(x[:, k][:, None] * y[:, k][None] for k in range(3))

    return dot(a[0], b[0]) + dot(a[1], b[1]), dot(a[1], b[0]) - dot(a[0], b[1])


def mul_left_adjoint(a, b):
    def dot(x, y):
        return sum(x[k][:, None] * y[k][None] for k in range(3))

    return dot(a[0], b[0]) + dot(a[1], b[1]), dot(a[0], b[1]) - dot(a[1], b[0])


def add(a, b):
    return b if a is None else (a[0] + b[0], a[1] + b[1])


def projected(m):
    r, i = m
    third = (i[0, 0] + i[1, 1] + i[2, 2]) / 3.0
    parts = [i[j, j] - third for j in range(3)]
    for j, k in ((0, 1), (0, 2), (1, 2)):
        parts += [(r[j, k] - r[k, j]) / 2.0, (i[j, k] + i[k, j]) / 2.0]
    return jnp.stack(parts)


def exponential(g):
    h = [g[0], g[1], g[2]]
    u, v, w = (g[3], g[4]), (g[5], g[6]), (g[7], g[8])
    nu, nv, nw = (z[0] * z[0] + z[1] * z[1] for z in (u, v, w))
    uw = (u[0] * w[0] - u[1] * w[1], u[0] * w[1] + u[1] * w[0])
    diag = [h[0] * h[0] + nu + nv, h[1] * h[1] + nu + nw, h[2] * h[2] + nv + nw]
    p = -0.5 * (diag[0] + diag[1] + diag[2])
    det = (
        h[0] * (h[1] * h[2] - nw)
        - h[1] * nv
        - h[2] * nu
        + 2.0 * (uw[1] * v[0] - uw[0] * v[1])
    )
    s01, s02, s12 = h[0] + h[1], h[0] + h[2], h[1] + h[2]
    square = {
        (0, 1): (
            -s01 * u[1] - (v[0] * w[0] + v[1] * w[1]),
            s01 * u[0] - (v[1] * w[0] - v[0] * w[1]),
        ),
        (0, 2): (-s02 * v[1] + uw[0], s02 * v[0] + uw[1]),
        (1, 2): (
            -s12 * w[1] - (u[0] * v[0] + u[1] * v[1]),
            s12 * w[0] - (u[0] * v[1] - u[1] * v[0]),
        ),
    }
    line = {(0, 1): u, (0, 2): v, (1, 2): w}
    ai4, br4 = det * (-1.0 / 120.0), 0.25 + p * (1.0 / 120.0)
    ai3, br3, bi3, cr3 = (
        det * (-1.0 / 60.0),
        1.0 / 3.0 + p * (1.0 / 60.0),
        ai4 * (1.0 / 3.0),
        br4 * (1.0 / 3.0),
    )
    ai2, br2, bi2, cr2, ci2 = (
        det * cr3 * -0.5,
        0.5 + 0.5 * p * cr3,
        0.5 * ai3,
        0.5 * br3,
        0.5 * bi3,
    )
    ar, ai = 1.0 + det * ci2, -det * cr2
    br, bi, cr, ci = 1.0 + p * cr2, ai2 + p * ci2, br2, bi2
    re = [[None] * 3 for _ in range(3)]
    im = [[None] * 3 for _ in range(3)]
    for j in range(3):
        re[j][j] = ar - bi * h[j] - cr * diag[j]
        im[j][j] = ai + br * h[j] - ci * diag[j]
    for j, k in line:
        x, s = line[j, k], square[j, k]
        even_r, odd_r = br * x[0], bi * x[1]
        even_i, odd_i = br * x[1], bi * x[0]
        cs = (cr * s[0], ci * s[1], cr * s[1], ci * s[0])
        re[j][k] = (even_r - odd_r) + (cs[0] - cs[1])
        im[j][k] = (even_i + odd_i) + (cs[2] + cs[3])
        re[k][j] = -(even_r + odd_r) + (cs[0] + cs[1])
        im[k][j] = (even_i - odd_i) + (cs[3] - cs[2])
    return (
        jnp.stack([jnp.stack(row) for row in re]),
        jnp.stack([jnp.stack(row) for row in im]),
    )


def runs(pairs):
    out = []
    for to, frm in pairs:
        if out and to == out[-1][0] + out[-1][2] and frm == out[-1][1] + out[-1][2]:
            out[-1][2] += 1
        else:
            out.append([to, frm, 1])
    return out


def neighbour_rows(block, offset):
    lx, ly, lt = block
    found = {}
    for row in range(lx * ly * lt):
        site = (row // (ly * lt), row // lt % ly, row % lt)
        moved = [site[k] + offset[k] for k in range(3)]
        step = tuple(moved[k] // block[k] for k in range(3))
        at = [moved[k] % block[k] for k in range(3)]
        frm = (at[0] * ly + at[1]) * lt + at[2]
        found.setdefault(step, []).append((row, frm))
    return found


def unit(k, sign):
    return tuple(sign if j == k else 0 for j in range(3))


CORNERS = [(m, n) for m in range(3) for n in range(3) if m != n]


def plan_of(block):
    remote, local = [], []
    for k in range(3):
        for kind, sign in (("minus", -1), ("plus", 1)):
            spans = [(0, 4)]
            if kind == "plus":
                spans = [(a, b) for a, b in ((0, k), (k + 1, 4)) if b > a]
            for step, pairs in neighbour_rows(block, unit(k, sign)).items():
                for to, frm, n in runs(pairs):
                    for a, b in spans:
                        item = (kind, k, a, b - a, to, frm, n)
                        if any(step):
                            remote.append(item + (step,))
                        else:
                            local.append(item)
    inner = []
    for c, (m, n) in enumerate(CORNERS):
        ahead, behind = unit(m, 1), unit(n, -1)
        rows_ahead = dict(neighbour_rows(block, ahead).get((0, 0, 0), []))
        rows_behind = dict(neighbour_rows(block, behind).get((0, 0, 0), []))
        offset = tuple(ahead[j] + behind[j] for j in range(3))
        from_minus, from_plus = [], []
        for step, pairs in neighbour_rows(block, offset).items():
            outer = []
            for to, frm in pairs:
                if to in rows_ahead:
                    from_minus.append((to, rows_ahead[to]))
                elif to in rows_behind:
                    from_plus.append((to, rows_behind[to]))
                else:
                    outer.append((to, frm))
            for to, frm, count in runs(outer):
                remote.append(("corner", c, n, 1, to, frm, count, step))
        for to, frm, count in runs(sorted(from_minus)):
            inner.append((c, "minus", n, n, to, frm, count))
        for to, frm, count in runs(sorted(from_plus)):
            inner.append((c, "plus", m, n, to, frm, count))
    return remote, local, inner


def kernel(
    block,
    sizes,
    plan,
    partners,
    w_ref,
    out_ref,
    act_ref,
    cur_ref,
    plus_ref,
    minus_ref,
    corner_ref,
    gen_ref,
    part_ref,
    slot_ref,
    send_sem,
    recv_sem,
    act_send,
    act_recv,
):
    remote, local, inner = plan
    rows = block[0] * block[1] * block[2]
    lanes = w_ref.shape[-1]
    here = [lax.axis_index(axis) for axis in AXES]

    def device(step):
        return tuple(lax.rem(here[k] + step[k] + sizes[k], sizes[k]) for k in range(3))

    steps = sorted({item[-1] for item in remote})
    greeted = steps + partners
    barrier = pltpu.get_barrier_semaphore()
    for step in greeted:
        pl.semaphore_signal(barrier, inc=1, device_id=device(step), device_id_type=MESH)
    pl.semaphore_wait(barrier, len(greeted))

    side = {"plus": plus_ref, "minus": minus_ref}
    action_copies = []

    for stage in range(3):
        field = w_ref if stage == 0 else cur_ref.at[stage - 1]
        copies = []
        for j, (kind, index, first, dirs, to, frm, count, step) in enumerate(remote):
            if kind == "corner":
                dst = corner_ref.at[stage, pl.ds(index, 1), :, :, :, pl.ds(to, count), :]
            else:
                dst = side[kind].at[
                    stage, index, pl.ds(first, dirs), :, :, :, pl.ds(to, count), :
                ]
            copy = pltpu.make_async_remote_copy(
                src_ref=field.at[pl.ds(first, dirs), :, :, :, pl.ds(frm, count), :],
                dst_ref=dst,
                send_sem=send_sem.at[stage, j],
                recv_sem=recv_sem.at[stage, j],
                device_id=device(tuple(-s for s in step)),
                device_id_type=MESH,
            )
            copy.start()
            copies.append(copy)
        for kind, index, first, dirs, to, frm, count in local:
            side[kind][stage, index, first : first + dirs, :, :, :, to : to + count, :] = field[
                first : first + dirs, :, :, :, frm : frm + count, :
            ]
        for copy in copies:
            copy.wait()
        for c, kind, index, n, to, frm, count in inner:
            corner_ref[stage, c, :, :, :, to : to + count, :] = side[kind][
                stage, index, n, :, :, :, frm : frm + count, :
            ]

        def centre(mu):
            return field[mu, 0], field[mu, 1]

        def roll(pair, shift):
            return tuple(pltpu.roll(x, shift % lanes, axis=3) for x in pair)

        def ahead(nu, mu):
            if mu == 3:
                return roll(centre(nu), -1)
            return plus_ref[stage, mu, nu, 0], plus_ref[stage, mu, nu, 1]

        def behind(mu, nu):
            return minus_ref[stage, nu, mu, 0], minus_ref[stage, nu, mu, 1]

        def corner(mu, nu):
            if mu == 3:
                return roll(behind(nu, nu), -1)
            c = CORNERS.index((mu, nu))
            return corner_ref[stage, c, 0], corner_ref[stage, c, 1]

        upper, lower = [None] * 4, [None] * 4
        action = None
        for mu in range(4):
            for nu in range(mu + 1, 4):
                one = mul(centre(mu), ahead(nu, mu))
                two = mul(centre(nu), ahead(mu, nu))
                plaq = mul_right_adjoint(one, two)
                if stage == 0:
                    trace = plaq[0][0, 0] + plaq[0][1, 1] + plaq[0][2, 2]
                    term = 1.0 - trace / 3.0
                    action = term if action is None else action + term
                flux = projected(plaq)
                upper[mu] = flux if upper[mu] is None else upper[mu] + flux
                upper[nu] = -flux if upper[nu] is None else upper[nu] - flux
                if nu == 3:
                    low = roll(mul_left_adjoint(one, centre(3)), 1)
                    lower[mu] = add(lower[mu], low)
        for mu in range(4):
            for nu in range(3):
                if nu != mu:
                    one = mul(behind(mu, nu), corner(mu, nu))
                    lower[mu] = add(lower[mu], mul_left_adjoint(one, behind(nu, nu)))
            omega = projected(mul(centre(mu), lower[mu])) + upper[mu]
            gen = (-flow_eps * FRESH[stage]) * omega
            if stage:
                gen = gen + KEPT[stage] * gen_ref[mu]
            if stage < 2:
                gen_ref[mu] = gen
            moved = mul(exponential(gen), centre(mu))
            if stage < 2:
                cur_ref[stage, mu, 0] = moved[0]
                cur_ref[stage, mu, 1] = moved[1]
            else:
                out_ref[mu, 0] = moved[0]
                out_ref[mu, 1] = moved[1]
        if stage == 0:
            lt = block[2]
            for t in range(lt):
                line = sum(action[r : r + 1] for r in range(t, rows, lt))
                part_ref[t : t + 1, :] = line
            mine = here[0] * sizes[1] + here[1]
            for j, step in enumerate(partners):
                copy = pltpu.make_async_remote_copy(
                    src_ref=part_ref,
                    dst_ref=slot_ref.at[mine],
                    send_sem=act_send.at[j],
                    recv_sem=act_recv.at[j],
                    device_id=device(step),
                    device_id_type=MESH,
                )
                copy.start()
                action_copies.append(copy)
            slot_ref[mine] = part_ref[...]
    for copy in action_copies:
        copy.wait()
    total = sum(slot_ref[j] for j in range(sizes[0] * sizes[1]))
    scale = 1.0 / (6.0 * sizes[0] * sizes[1] * block[0] * block[1] * lanes)
    total = jnp.sum(total, axis=1, keepdims=True) * scale
    act_ref[...] = jnp.broadcast_to(total, act_ref.shape)


def solution(mesh):
    sizes = tuple(mesh.shape[axis] for axis in AXES)

    def local(links):
        block = links.shape[4:7]
        lanes = links.shape[7]
        rows = block[0] * block[1] * block[2]
        plan = plan_of(block)
        partners = [
            (i, j, 0) for i in range(sizes[0]) for j in range(sizes[1]) if i or j
        ]
        count = len(plan[0])
        matrix = (2, 3, 3, rows, lanes)
        f32 = jnp.float32
        vmem = pl.BlockSpec(memory_space=pltpu.VMEM)
        flowed, action = pl.pallas_call(
            functools.partial(kernel, block, sizes, plan, partners),
            out_shape=(
                jax.ShapeDtypeStruct((4,) + matrix, f32),
                jax.ShapeDtypeStruct((block[2], lanes), f32),
            ),
            in_specs=[vmem],
            out_specs=(vmem, vmem),
            scratch_shapes=[
                pltpu.VMEM((2, 4) + matrix, f32),
                pltpu.VMEM((3, 3, 4) + matrix, f32),
                pltpu.VMEM((3, 3, 4) + matrix, f32),
                pltpu.VMEM((3, len(CORNERS)) + matrix, f32),
                pltpu.VMEM((4, 9, rows, lanes), f32),
                pltpu.VMEM((block[2], lanes), f32),
                pltpu.VMEM((sizes[0] * sizes[1], block[2], lanes), f32),
                pltpu.SemaphoreType.DMA((3, count)),
                pltpu.SemaphoreType.DMA((3, count)),
                pltpu.SemaphoreType.DMA((len(partners),)),
                pltpu.SemaphoreType.DMA((len(partners),)),
            ],
            compiler_params=pltpu.CompilerParams(
                collective_id=0, has_side_effects=True, vmem_limit_bytes=48 * 2**20
            ),
        )(links.reshape((4,) + matrix))
        return flowed.reshape(links.shape), action[:, 0]

    spec = P(None, None, None, None, "gx", "gy", "ta", None)
    return jax.shard_map(
        local, mesh=mesh, in_specs=(spec,), out_specs=(spec, P("ta")), check_vma=False
    )
```

```python
import functools

import jax
import jax.numpy as jnp
from jax import lax
from jax.experimental import pallas as pl
from jax.experimental.pallas import tpu as pltpu
from jax.sharding import PartitionSpec as P

MESH = pl.DeviceIdType.MESH
AXES = ("gx", "gy", "ta")
flow_eps = 0.1
FRESH = (1.0 / 4.0, 8.0 / 9.0, 3.0 / 4.0)
KEPT = (0.0, -17.0 / 9.0, -1.0)


def mul(a, b):
    def dot(x, y):
        return sum(x[:, k][:, None] * y[k][None] for k in range(3))

    return dot(a[0], b[0]) - dot(a[1], b[1]), dot(a[0], b[1]) + dot(a[1], b[0])


def mul_right_adjoint(a, b):
    def dot(x, y):
        return sum(x[:, k][:, None] * y[:, k][None] for k in range(3))

    return dot(a[0], b[0]) + dot(a[1], b[1]), dot(a[1], b[0]) - dot(a[0], b[1])


def mul_left_adjoint(a, b):
    def dot(x, y):
        return sum(x[k][:, None] * y[k][None] for k in range(3))

    return dot(a[0], b[0]) + dot(a[1], b[1]), dot(a[0], b[1]) - dot(a[1], b[0])


def add(a, b):
    return b if a is None else (a[0] + b[0], a[1] + b[1])


def projected(m):
    r, i = m
    third = (i[0, 0] + i[1, 1] + i[2, 2]) / 3.0
    parts = [i[j, j] - third for j in range(2)]
    for j, k in ((0, 1), (0, 2), (1, 2)):
        parts += [(r[j, k] - r[k, j]) / 2.0, (i[j, k] + i[k, j]) / 2.0]
    return jnp.stack(parts)


def exponential(g):
    h = [g[0], g[1], -(g[0] + g[1])]
    u, v, w = (g[2], g[3]), (g[4], g[5]), (g[6], g[7])
    nu, nv, nw = (z[0] * z[0] + z[1] * z[1] for z in (u, v, w))
    uw = (u[0] * w[0] - u[1] * w[1], u[0] * w[1] + u[1] * w[0])
    diag = [h[0] * h[0] + nu + nv, h[1] * h[1] + nu + nw, h[2] * h[2] + nv + nw]
    p = -0.5 * (diag[0] + diag[1] + diag[2])
    det = (
        h[0] * (h[1] * h[2] - nw)
        - h[1] * nv
        - h[2] * nu
        + 2.0 * (uw[1] * v[0] - uw[0] * v[1])
    )
    s01, s02, s12 = h[0] + h[1], h[0] + h[2], h[1] + h[2]
    square = {
        (0, 1): (
            -s01 * u[1] - (v[0] * w[0] + v[1] * w[1]),
            s01 * u[0] - (v[1] * w[0] - v[0] * w[1]),
        ),
        (0, 2): (-s02 * v[1] + uw[0], s02 * v[0] + uw[1]),
        (1, 2): (
            -s12 * w[1] - (u[0] * v[0] + u[1] * v[1]),
            s12 * w[0] - (u[0] * v[1] - u[1] * v[0]),
        ),
    }
    line = {(0, 1): u, (0, 2): v, (1, 2): w}
    ai4, br4 = det * (-1.0 / 120.0), 0.25 + p * (1.0 / 120.0)
    ai3, br3, bi3, cr3 = (
        det * (-1.0 / 60.0),
        1.0 / 3.0 + p * (1.0 / 60.0),
        ai4 * (1.0 / 3.0),
        br4 * (1.0 / 3.0),
    )
    ai2, br2, bi2, cr2, ci2 = (
        det * cr3 * -0.5,
        0.5 + 0.5 * p * cr3,
        0.5 * ai3,
        0.5 * br3,
        0.5 * bi3,
    )
    ar, ai = 1.0 + det * ci2, -det * cr2
    br, bi, cr, ci = 1.0 + p * cr2, ai2 + p * ci2, br2, bi2
    re = [[None] * 3 for _ in range(3)]
    im = [[None] * 3 for _ in range(3)]
    for j in range(3):
        re[j][j] = ar - bi * h[j] - cr * diag[j]
        im[j][j] = ai + br * h[j] - ci * diag[j]
    for j, k in line:
        x, s = line[j, k], square[j, k]
        even_r, odd_r = br * x[0], bi * x[1]
        even_i, odd_i = br * x[1], bi * x[0]
        cs = (cr * s[0], ci * s[1], cr * s[1], ci * s[0])
        re[j][k] = (even_r - odd_r) + (cs[0] - cs[1])
        im[j][k] = (even_i + odd_i) + (cs[2] + cs[3])
        re[k][j] = -(even_r + odd_r) + (cs[0] + cs[1])
        im[k][j] = (even_i - odd_i) + (cs[3] - cs[2])
    return (
        jnp.stack([jnp.stack(row) for row in re]),
        jnp.stack([jnp.stack(row) for row in im]),
    )


def runs(pairs):
    out = []
    for to, frm in pairs:
        if out and to == out[-1][0] + out[-1][2] and frm == out[-1][1] + out[-1][2]:
            out[-1][2] += 1
        else:
            out.append([to, frm, 1])
    return out


def neighbour_rows(block, offset):
    lx, ly, lt = block
    found = {}
    for row in range(lx * ly * lt):
        site = (row // (ly * lt), row // lt % ly, row % lt)
        moved = [site[k] + offset[k] for k in range(3)]
        step = tuple(moved[k] // block[k] for k in range(3))
        at = [moved[k] % block[k] for k in range(3)]
        frm = (at[0] * ly + at[1]) * lt + at[2]
        found.setdefault(step, []).append((row, frm))
    return found


def unit(k, sign):
    return tuple(sign if j == k else 0 for j in range(3))


PAIRS = [(0, 1), (0, 2), (1, 2)]


def place(m, n):
    return PAIRS.index((min(m, n), max(m, n))), int(m > n)


def plan_of(block):
    remote, local = [], []
    for k in range(3):
        for half, sign in ((0, -1), (1, 1)):
            spans = [(0, 4)]
            if half:
                spans = [(a, b) for a, b in ((0, k), (k + 1, 4)) if b > a]
            for step, pairs in neighbour_rows(block, unit(k, sign)).items():
                for to, frm, n in runs(pairs):
                    for a, b in spans:
                        item = (int(k == 2), "face", k, half, a, b - a, to, frm, n)
                        if any(step):
                            remote.append(item + (step,))
                        else:
                            local.append(item)
    inner = []
    for m in range(3):
        for n in range(3):
            if m == n:
                continue
            c, half = place(m, n)
            ahead, behind = unit(m, 1), unit(n, -1)
            rows_ahead = dict(neighbour_rows(block, ahead).get((0, 0, 0), []))
            rows_behind = dict(neighbour_rows(block, behind).get((0, 0, 0), []))
            offset = tuple(ahead[j] + behind[j] for j in range(3))
            group = int(2 in (m, n))
            from_minus, from_plus = [], []
            for step, pairs in neighbour_rows(block, offset).items():
                outer = []
                for to, frm in pairs:
                    if to in rows_ahead:
                        from_minus.append((to, rows_ahead[to]))
                    elif to in rows_behind:
                        from_plus.append((to, rows_behind[to]))
                    else:
                        outer.append((to, frm))
                for to, frm, count in runs(outer):
                    remote.append((group, "corner", c, half, n, 1, to, frm, count, step))
            for to, frm, count in runs(sorted(from_minus)):
                inner.append((group, c, half, n, 0, n, to, frm, count))
            for to, frm, count in runs(sorted(from_plus)):
                inner.append((group, c, half, m, 1, n, to, frm, count))
    remote.sort(key=lambda item: -item[0])
    return remote, local, inner


def kernel(
    block,
    sizes,
    plan,
    partners,
    w_ref,
    out_ref,
    act_ref,
    cur_ref,
    face_ref,
    corner_ref,
    gen_ref,
    gen_face_ref,
    gen_corner_ref,
    part_ref,
    slot_ref,
    send_sem,
    recv_sem,
    act_send,
    act_recv,
):
    remote, local, inner = plan
    rows = block[0] * block[1] * block[2]
    lanes = w_ref.shape[-1]
    here = [lax.axis_index(axis) for axis in AXES]

    def device(step):
        return tuple(lax.rem(here[k] + step[k] + sizes[k], sizes[k]) for k in range(3))

    steps = sorted({item[-1] for item in remote})
    greeted = steps + partners
    barrier = pltpu.get_barrier_semaphore()
    for step in greeted:
        pl.semaphore_signal(barrier, inc=1, device_id=device(step), device_id_type=MESH)
    pl.semaphore_wait(barrier, len(greeted))

    started, action_copies = [], []

    for stage in range(3):
        field = w_ref if stage == 0 else cur_ref.at[stage - 1]
        copies = []
        for j, item in enumerate(remote):
            group, kind, index, half, first, dirs, to, frm, count, step = item
            span, put, take = pl.ds(first, dirs), pl.ds(half * rows + to, count), pl.ds(frm, count)
            if stage == 0:
                src = w_ref.at[span, :, pl.ds(0, 2), :, take, :]
                if kind == "corner":
                    dst = corner_ref.at[pl.ds(index, 1), :, pl.ds(0, 2), :, put, :]
                else:
                    dst = face_ref.at[index, span, :, pl.ds(0, 2), :, put, :]
            else:
                src = gen_ref.at[stage - 1, span, :, take, :]
                if kind == "corner":
                    dst = gen_corner_ref.at[stage - 1, pl.ds(index, 1), :, put, :]
                else:
                    dst = gen_face_ref.at[stage - 1, index, span, :, put, :]
            copy = pltpu.make_async_remote_copy(
                src_ref=src,
                dst_ref=dst,
                send_sem=send_sem.at[stage, j],
                recv_sem=recv_sem.at[stage, j],
                device_id=device(tuple(-s for s in step)),
                device_id_type=MESH,
            )
            copy.start()
            copies.append((group, copy))
            started.append(copy)
        for group, kind, index, half, first, dirs, to, frm, count in local:
            low = half * rows + to
            if stage == 0:
                face_ref[index, first : first + dirs, :, 0:2, :, low : low + count, :] = w_ref[
                    first : first + dirs, :, 0:2, :, frm : frm + count, :
                ]
            else:
                gen_face_ref[stage - 1, index, first : first + dirs, :, low : low + count, :] = (
                    gen_ref[stage - 1, first : first + dirs, :, frm : frm + count, :]
                )

        def renew(ref, generator):
            if stage == 0:
                r, i = ref[0, 0:2], ref[1, 0:2]
                for j in range(3):
                    k, l = (j + 1) % 3, (j + 2) % 3
                    ref[0, 2, j] = (r[0, k] * r[1, l] - i[0, k] * i[1, l]) - (
                        r[0, l] * r[1, k] - i[0, l] * i[1, k]
                    )
                    ref[1, 2, j] = (r[0, l] * i[1, k] + i[0, l] * r[1, k]) - (
                        r[0, k] * i[1, l] + i[0, k] * r[1, l]
                    )
            else:
                new = mul(exponential(generator[...]), (ref[0], ref[1]))
                ref[0] = new[0]
                ref[1] = new[1]

        def arrive(wanted):
            for group, copy in copies:
                if group == wanted:
                    copy.wait_recv()
            for k in (0, 1) if wanted == 0 else (2,):
                for mu in range(4):
                    renew(face_ref.at[k, mu], gen_face_ref.at[max(stage - 1, 0), k, mu])
            for c, pair in enumerate(PAIRS):
                if int(2 in pair) == wanted:
                    renew(corner_ref.at[c], gen_corner_ref.at[max(stage - 1, 0), c])
            for group, c, half, k, side, n, to, frm, count in inner:
                if group == wanted:
                    put, take = half * rows + to, side * rows + frm
                    corner_ref[c, :, :, :, put : put + count, :] = face_ref[
                        k, n, :, :, :, take : take + count, :
                    ]

        def centre(mu):
            return field[mu, 0], field[mu, 1]

        def roll(pair, shift):
            return tuple(pltpu.roll(x, shift % lanes, axis=3) for x in pair)

        def part(ref, index, half):
            low = half * rows
            return tuple(ref[index + (c, slice(None), slice(None), slice(low, low + rows))] for c in range(2))

        def ahead(nu, mu):
            return roll(centre(nu), -1) if mu == 3 else part(face_ref, (mu, nu), 1)

        def behind(mu, nu):
            return part(face_ref, (nu, mu), 0)

        def corner(mu, nu):
            if mu == 3:
                return roll(behind(nu, nu), -1)
            c, half = place(mu, nu)
            return part(corner_ref, (c,), half)

        upper, lower = [None] * 4, [None] * 4
        action = None
        for wanted in (0, 1):
            arrive(wanted)
            for mu in range(4):
                for nu in range(mu + 1, 4):
                    if int(2 in (mu, nu)) != wanted:
                        continue
                    one = mul(centre(mu), ahead(nu, mu))
                    two = mul(centre(nu), ahead(mu, nu))
                    plaq = mul_right_adjoint(one, two)
                    if stage == 0:
                        trace = plaq[0][0, 0] + plaq[0][1, 1] + plaq[0][2, 2]
                        term = 1.0 - trace / 3.0
                        action = term if action is None else action + term
                    flux = projected(plaq)
                    upper[mu] = flux if upper[mu] is None else upper[mu] + flux
                    upper[nu] = -flux if upper[nu] is None else upper[nu] - flux
                    if nu == 3:
                        low = roll(mul_left_adjoint(one, centre(3)), 1)
                        lower[mu] = add(lower[mu], low)
            for mu in range(4):
                for nu in range(3):
                    if nu != mu and int(2 in (mu, nu)) == wanted:
                        one = mul(behind(mu, nu), corner(mu, nu))
                        lower[mu] = add(lower[mu], mul_left_adjoint(one, behind(nu, nu)))
        for mu in range(4):
            omega = projected(mul(centre(mu), lower[mu])) + upper[mu]
            gen = (-flow_eps * FRESH[stage]) * omega
            if stage:
                gen = gen + KEPT[stage] * gen_ref[stage - 1, mu]
            if stage < 2:
                gen_ref[stage, mu] = gen
            moved = mul(exponential(gen), centre(mu))
            if stage < 2:
                cur_ref[stage, mu, 0] = moved[0]
                cur_ref[stage, mu, 1] = moved[1]
            else:
                out_ref[mu, 0] = moved[0]
                out_ref[mu, 1] = moved[1]
        if stage == 0:
            lt = block[2]
            for t in range(lt):
                line = sum(action[r : r + 1] for r in range(t, rows, lt))
                part_ref[t : t + 1, :] = line
            mine = here[0] * sizes[1] + here[1]
            for j, step in enumerate(partners):
                copy = pltpu.make_async_remote_copy(
                    src_ref=part_ref,
                    dst_ref=slot_ref.at[mine],
                    send_sem=act_send.at[j],
                    recv_sem=act_recv.at[j],
                    device_id=device(step),
                    device_id_type=MESH,
                )
                copy.start()
                action_copies.append(copy)
            slot_ref[mine] = part_ref[...]
    for copy in started:
        copy.wait_send()
    for copy in action_copies:
        copy.wait()
    total = sum(slot_ref[j] for j in range(sizes[0] * sizes[1]))
    scale = 1.0 / (6.0 * sizes[0] * sizes[1] * block[0] * block[1] * lanes)
    total = jnp.sum(total, axis=1, keepdims=True) * scale
    act_ref[...] = jnp.broadcast_to(total, act_ref.shape)


def solution(mesh):
    sizes = tuple(mesh.shape[axis] for axis in AXES)

    def local(links):
        block = links.shape[4:7]
        lanes = links.shape[7]
        rows = block[0] * block[1] * block[2]
        plan = plan_of(block)
        partners = [
            (i, j, 0) for i in range(sizes[0]) for j in range(sizes[1]) if i or j
        ]
        count = len(plan[0])
        matrix = (2, 3, 3, rows, lanes)
        both = (2, 3, 3, 2 * rows, lanes)
        f32 = jnp.float32
        vmem = pl.BlockSpec(memory_space=pltpu.VMEM)
        flowed, action = pl.pallas_call(
            functools.partial(kernel, block, sizes, plan, partners),
            out_shape=(
                jax.ShapeDtypeStruct((4,) + matrix, f32),
                jax.ShapeDtypeStruct((block[2], lanes), f32),
            ),
            in_specs=[vmem],
            out_specs=(vmem, vmem),
            scratch_shapes=[
                pltpu.VMEM((2, 4) + matrix, f32),
                pltpu.VMEM((3, 4) + both, f32),
                pltpu.VMEM((len(PAIRS),) + both, f32),
                pltpu.VMEM((2, 4, 8, rows, lanes), f32),
                pltpu.VMEM((2, 3, 4, 8, 2 * rows, lanes), f32),
                pltpu.VMEM((2, len(PAIRS), 8, 2 * rows, lanes), f32),
                pltpu.VMEM((block[2], lanes), f32),
                pltpu.VMEM((sizes[0] * sizes[1], block[2], lanes), f32),
                pltpu.SemaphoreType.DMA((3, count)),
                pltpu.SemaphoreType.DMA((3, count)),
                pltpu.SemaphoreType.DMA((len(partners),)),
                pltpu.SemaphoreType.DMA((len(partners),)),
            ],
            compiler_params=pltpu.CompilerParams(
                collective_id=0, has_side_effects=True, vmem_limit_bytes=48 * 2**20
            ),
        )(links.reshape((4,) + matrix))
        return flowed.reshape(links.shape), action[:, 0]

    spec = P(None, None, None, None, "gx", "gy", "ta", None)
    return jax.shard_map(
        local, mesh=mesh, in_specs=(spec,), out_specs=(spec, P("ta")), check_vma=False
    )
```

```python
import functools

import jax
import jax.numpy as jnp
from jax import lax
from jax.experimental import pallas as pl
from jax.experimental.pallas import tpu as pltpu
from jax.sharding import PartitionSpec as P

MESH = pl.DeviceIdType.MESH
AXES = ("gx", "gy", "ta")
flow_eps = 0.1
FRESH = (1.0 / 4.0, 8.0 / 9.0, 3.0 / 4.0)
KEPT = (0.0, -17.0 / 9.0, -1.0)


def mul(a, b):
    def dot(x, y):
        return sum(x[:, k][:, None] * y[k][None] for k in range(3))

    return dot(a[0], b[0]) - dot(a[1], b[1]), dot(a[0], b[1]) + dot(a[1], b[0])


def mul_right_adjoint(a, b):
    def dot(x, y):
        return sum(x[:, k][:, None] * y[:, k][None] for k in range(3))

    return dot(a[0], b[0]) + dot(a[1], b[1]), dot(a[1], b[0]) - dot(a[0], b[1])


def mul_left_adjoint(a, b):
    def dot(x, y):
        return sum(x[k][:, None] * y[k][None] for k in range(3))

    return dot(a[0], b[0]) + dot(a[1], b[1]), dot(a[0], b[1]) - dot(a[1], b[0])


def add(a, b):
    return b if a is None else (a[0] + b[0], a[1] + b[1])


def projected(m):
    r, i = m
    third = (i[0, 0] + i[1, 1] + i[2, 2]) / 3.0
    parts = [i[j, j] - third for j in range(2)]
    for j, k in ((0, 1), (0, 2), (1, 2)):
        parts += [(r[j, k] - r[k, j]) / 2.0, (i[j, k] + i[k, j]) / 2.0]
    return jnp.stack(parts)


def exponential(g):
    h = [g[0], g[1], -(g[0] + g[1])]
    u, v, w = (g[2], g[3]), (g[4], g[5]), (g[6], g[7])
    nu, nv, nw = (z[0] * z[0] + z[1] * z[1] for z in (u, v, w))
    uw = (u[0] * w[0] - u[1] * w[1], u[0] * w[1] + u[1] * w[0])
    diag = [h[0] * h[0] + nu + nv, h[1] * h[1] + nu + nw, h[2] * h[2] + nv + nw]
    p = -0.5 * (diag[0] + diag[1] + diag[2])
    det = (
        h[0] * (h[1] * h[2] - nw)
        - h[1] * nv
        - h[2] * nu
        + 2.0 * (uw[1] * v[0] - uw[0] * v[1])
    )
    s01, s02, s12 = h[0] + h[1], h[0] + h[2], h[1] + h[2]
    square = {
        (0, 1): (
            -s01 * u[1] - (v[0] * w[0] + v[1] * w[1]),
            s01 * u[0] - (v[1] * w[0] - v[0] * w[1]),
        ),
        (0, 2): (-s02 * v[1] + uw[0], s02 * v[0] + uw[1]),
        (1, 2): (
            -s12 * w[1] - (u[0] * v[0] + u[1] * v[1]),
            s12 * w[0] - (u[0] * v[1] - u[1] * v[0]),
        ),
    }
    line = {(0, 1): u, (0, 2): v, (1, 2): w}
    ai4, br4 = det * (-1.0 / 120.0), 0.25 + p * (1.0 / 120.0)
    ai3, br3, bi3, cr3 = (
        det * (-1.0 / 60.0),
        1.0 / 3.0 + p * (1.0 / 60.0),
        ai4 * (1.0 / 3.0),
        br4 * (1.0 / 3.0),
    )
    ai2, br2, bi2, cr2, ci2 = (
        det * cr3 * -0.5,
        0.5 + 0.5 * p * cr3,
        0.5 * ai3,
        0.5 * br3,
        0.5 * bi3,
    )
    ar, ai = 1.0 + det * ci2, -det * cr2
    br, bi, cr, ci = 1.0 + p * cr2, ai2 + p * ci2, br2, bi2
    re = [[None] * 3 for _ in range(3)]
    im = [[None] * 3 for _ in range(3)]
    for j in range(3):
        re[j][j] = ar - bi * h[j] - cr * diag[j]
        im[j][j] = ai + br * h[j] - ci * diag[j]
    for j, k in line:
        x, s = line[j, k], square[j, k]
        even_r, odd_r = br * x[0], bi * x[1]
        even_i, odd_i = br * x[1], bi * x[0]
        cs = (cr * s[0], ci * s[1], cr * s[1], ci * s[0])
        re[j][k] = (even_r - odd_r) + (cs[0] - cs[1])
        im[j][k] = (even_i + odd_i) + (cs[2] + cs[3])
        re[k][j] = -(even_r + odd_r) + (cs[0] + cs[1])
        im[k][j] = (even_i - odd_i) + (cs[3] - cs[2])
    return (
        jnp.stack([jnp.stack(row) for row in re]),
        jnp.stack([jnp.stack(row) for row in im]),
    )


def runs(pairs):
    out = []
    for to, frm in pairs:
        if out and to == out[-1][0] + out[-1][2] and frm == out[-1][1] + out[-1][2]:
            out[-1][2] += 1
        else:
            out.append([to, frm, 1])
    return out


def neighbour_rows(block, offset):
    lx, ly, lt = block
    found = {}
    for row in range(lx * ly * lt):
        site = (row // (ly * lt), row // lt % ly, row % lt)
        moved = [site[k] + offset[k] for k in range(3)]
        step = tuple(moved[k] // block[k] for k in range(3))
        at = [moved[k] % block[k] for k in range(3)]
        frm = (at[0] * ly + at[1]) * lt + at[2]
        found.setdefault(step, []).append((row, frm))
    return found


def unit(k, sign):
    return tuple(sign if j == k else 0 for j in range(3))


PAIRS = [(0, 1), (0, 2), (1, 2)]


def place(m, n):
    return PAIRS.index((min(m, n), max(m, n))), int(m > n)


def plan_of(block):
    remote, local = [], []
    for k in range(3):
        for half, sign in ((0, -1), (1, 1)):
            spans = [(0, 4)]
            if half:
                spans = [(a, b) for a, b in ((0, k), (k + 1, 4)) if b > a]
            for step, pairs in neighbour_rows(block, unit(k, sign)).items():
                for to, frm, n in runs(pairs):
                    for a, b in spans:
                        item = (int(k == 2), "face", k, half, a, b - a, to, frm, n)
                        if any(step):
                            remote.append(item + (step,))
                        else:
                            local.append(item)
    inner = []
    for m in range(3):
        for n in range(3):
            if m == n:
                continue
            c, half = place(m, n)
            ahead, behind = unit(m, 1), unit(n, -1)
            rows_ahead = dict(neighbour_rows(block, ahead).get((0, 0, 0), []))
            rows_behind = dict(neighbour_rows(block, behind).get((0, 0, 0), []))
            offset = tuple(ahead[j] + behind[j] for j in range(3))
            group = 2 * int(2 in (m, n))
            from_minus, from_plus = [], []
            for step, pairs in neighbour_rows(block, offset).items():
                outer = []
                for to, frm in pairs:
                    if to in rows_ahead:
                        from_minus.append((to, rows_ahead[to]))
                    elif to in rows_behind:
                        from_plus.append((to, rows_behind[to]))
                    else:
                        outer.append((to, frm))
                for to, frm, count in runs(outer):
                    remote.append((group, "corner", c, half, n, 1, to, frm, count, step))
            for to, frm, count in runs(sorted(from_minus)):
                inner.append((group, c, half, n, 0, n, to, frm, count))
            for to, frm, count in runs(sorted(from_plus)):
                inner.append((group, c, half, m, 1, n, to, frm, count))
    remote.sort(key=lambda item: (item[1] == "face", -item[0]))
    return remote, local, inner


def kernel(
    block,
    sizes,
    plan,
    partners,
    w_hbm,
    out_ref,
    act_ref,
    w_ref,
    cur_ref,
    face_ref,
    corner_ref,
    gen_ref,
    gen_face_ref,
    gen_corner_ref,
    part_ref,
    slot_ref,
    send_sem,
    recv_sem,
    act_send,
    act_recv,
    load_sem,
):
    remote, local, inner = plan
    rows = block[0] * block[1] * block[2]
    lanes = w_hbm.shape[-1]
    load = pltpu.make_async_copy(w_hbm, w_ref, load_sem)
    load.start()
    here = [lax.axis_index(axis) for axis in AXES]

    def device(step):
        return tuple(lax.rem(here[k] + step[k] + sizes[k], sizes[k]) for k in range(3))

    steps = sorted({item[-1] for item in remote})
    greeted = steps + partners
    barrier = pltpu.get_barrier_semaphore()
    for step in greeted:
        pl.semaphore_signal(barrier, inc=1, device_id=device(step), device_id_type=MESH)
    pl.semaphore_wait(barrier, len(greeted))
    load.wait()

    started, action_copies = [], []

    for stage in range(3):
        field = w_ref if stage == 0 else cur_ref.at[stage - 1]
        copies = []
        for j, item in enumerate(remote):
            group, kind, index, half, first, dirs, to, frm, count, step = item
            span, put, take = pl.ds(first, dirs), pl.ds(half * rows + to, count), pl.ds(frm, count)
            if stage == 0:
                src = w_ref.at[span, :, pl.ds(0, 2), :, take, :]
                if kind == "corner":
                    dst = corner_ref.at[pl.ds(index, 1), :, pl.ds(0, 2), :, put, :]
                else:
                    dst = face_ref.at[index, span, :, pl.ds(0, 2), :, put, :]
            else:
                src = gen_ref.at[stage - 1, span, :, take, :]
                if kind == "corner":
                    dst = gen_corner_ref.at[stage - 1, pl.ds(index, 1), :, put, :]
                else:
                    dst = gen_face_ref.at[stage - 1, index, span, :, put, :]
            copy = pltpu.make_async_remote_copy(
                src_ref=src,
                dst_ref=dst,
                send_sem=send_sem.at[stage, j],
                recv_sem=recv_sem.at[stage, j],
                device_id=device(tuple(-s for s in step)),
                device_id_type=MESH,
            )
            copy.start()
            copies.append((group, copy))
            started.append(copy)
        if stage:
            before = w_ref if stage == 1 else cur_ref.at[stage - 2]
            for mu in range(4):
                own = (before[mu, 0], before[mu, 1])
                moved = mul(exponential(gen_ref[stage - 1, mu]), own)
                cur_ref[stage - 1, mu, 0] = moved[0]
                cur_ref[stage - 1, mu, 1] = moved[1]
        if stage == 1:
            lt = block[2]
            for t in range(lt):
                line = sum(action[r : r + 1] for r in range(t, rows, lt))
                part_ref[t : t + 1, :] = line
            mine = here[0] * sizes[1] + here[1]
            for j, step in enumerate(partners):
                copy = pltpu.make_async_remote_copy(
                    src_ref=part_ref,
                    dst_ref=slot_ref.at[mine],
                    send_sem=act_send.at[j],
                    recv_sem=act_recv.at[j],
                    device_id=device(step),
                    device_id_type=MESH,
                )
                copy.start()
                action_copies.append(copy)
            slot_ref[mine] = part_ref[...]
        for group, kind, index, half, first, dirs, to, frm, count in local:
            low = half * rows + to
            if stage == 0:
                face_ref[index, first : first + dirs, :, 0:2, :, low : low + count, :] = w_ref[
                    first : first + dirs, :, 0:2, :, frm : frm + count, :
                ]
            else:
                gen_face_ref[stage - 1, index, first : first + dirs, :, low : low + count, :] = (
                    gen_ref[stage - 1, first : first + dirs, :, frm : frm + count, :]
                )

        def renew(ref, generator):
            if stage == 0:
                r, i = ref[0, 0:2], ref[1, 0:2]
                for j in range(3):
                    k, l = (j + 1) % 3, (j + 2) % 3
                    ref[0, 2, j] = (r[0, k] * r[1, l] - i[0, k] * i[1, l]) - (
                        r[0, l] * r[1, k] - i[0, l] * i[1, k]
                    )
                    ref[1, 2, j] = (r[0, l] * i[1, k] + i[0, l] * r[1, k]) - (
                        r[0, k] * i[1, l] + i[0, k] * r[1, l]
                    )
            else:
                new = mul(exponential(generator[...]), (ref[0], ref[1]))
                ref[0] = new[0]
                ref[1] = new[1]

        def arrive(wanted):
            for group, copy in copies:
                if group == wanted:
                    copy.wait_recv()
            for k in ((0, 1), (2,), ())[wanted]:
                for mu in range(4):
                    renew(face_ref.at[k, mu], gen_face_ref.at[max(stage - 1, 0), k, mu])
            for c, pair in enumerate(PAIRS):
                if 2 * int(2 in pair) == wanted:
                    renew(corner_ref.at[c], gen_corner_ref.at[max(stage - 1, 0), c])
            for group, c, half, k, side, n, to, frm, count in inner:
                if group == wanted:
                    put, take = half * rows + to, side * rows + frm
                    corner_ref[c, :, :, :, put : put + count, :] = face_ref[
                        k, n, :, :, :, take : take + count, :
                    ]

        def centre(mu):
            return field[mu, 0], field[mu, 1]

        def roll(pair, shift):
            return tuple(pltpu.roll(x, shift % lanes, axis=3) for x in pair)

        def part(ref, index, half):
            low = half * rows
            return tuple(ref[index + (c, slice(None), slice(None), slice(low, low + rows))] for c in range(2))

        def ahead(nu, mu):
            return roll(centre(nu), -1) if mu == 3 else part(face_ref, (mu, nu), 1)

        def behind(mu, nu):
            return part(face_ref, (nu, mu), 0)

        def corner(mu, nu):
            if mu == 3:
                return roll(behind(nu, nu), -1)
            c, half = place(mu, nu)
            return part(corner_ref, (c,), half)

        upper, lower = [None] * 4, [None] * 4
        if stage == 0:
            action = None
        for wanted in (0, 1, 2):
            arrive(wanted)
            for mu in range(4):
                for nu in range(mu + 1, 4):
                    if int(2 in (mu, nu)) != wanted:
                        continue
                    one = mul(centre(mu), ahead(nu, mu))
                    two = mul(centre(nu), ahead(mu, nu))
                    plaq = mul_right_adjoint(one, two)
                    if stage == 0:
                        trace = plaq[0][0, 0] + plaq[0][1, 1] + plaq[0][2, 2]
                        term = 1.0 - trace / 3.0
                        action = term if action is None else action + term
                    flux = projected(plaq)
                    upper[mu] = flux if upper[mu] is None else upper[mu] + flux
                    upper[nu] = -flux if upper[nu] is None else upper[nu] - flux
                    if nu == 3:
                        low = roll(mul_left_adjoint(one, centre(3)), 1)
                        lower[mu] = add(lower[mu], low)
            for mu in range(4):
                for nu in range(3):
                    late = int(2 in (mu, nu)) * (1 if mu == 3 else 2)
                    if nu != mu and late == wanted:
                        one = mul(behind(mu, nu), corner(mu, nu))
                        lower[mu] = add(lower[mu], mul_left_adjoint(one, behind(nu, nu)))
            for mu in ((), (3,), (0, 1, 2))[wanted]:
                omega = projected(mul(centre(mu), lower[mu])) + upper[mu]
                gen = (-flow_eps * FRESH[stage]) * omega
                if stage:
                    gen = gen + KEPT[stage] * gen_ref[stage - 1, mu]
                if stage < 2:
                    gen_ref[stage, mu] = gen
                else:
                    moved = mul(exponential(gen), centre(mu))
                    out_ref[mu, 0] = moved[0]
                    out_ref[mu, 1] = moved[1]
    for copy in started:
        copy.wait_send()
    for copy in action_copies:
        copy.wait()
    total = sum(slot_ref[j] for j in range(sizes[0] * sizes[1]))
    scale = 1.0 / (6.0 * sizes[0] * sizes[1] * block[0] * block[1] * lanes)
    total = jnp.sum(total, axis=1, keepdims=True) * scale
    act_ref[...] = jnp.broadcast_to(total, act_ref.shape)


def solution(mesh):
    sizes = tuple(mesh.shape[axis] for axis in AXES)

    def local(links):
        block = links.shape[4:7]
        lanes = links.shape[7]
        rows = block[0] * block[1] * block[2]
        plan = plan_of(block)
        partners = [
            (i, j, 0) for i in range(sizes[0]) for j in range(sizes[1]) if i or j
        ]
        count = len(plan[0])
        matrix = (2, 3, 3, rows, lanes)
        both = (2, 3, 3, 2 * rows, lanes)
        f32 = jnp.float32
        vmem = pl.BlockSpec(memory_space=pltpu.VMEM)
        flowed, action = pl.pallas_call(
            functools.partial(kernel, block, sizes, plan, partners),
            out_shape=(
                jax.ShapeDtypeStruct((4,) + matrix, f32),
                jax.ShapeDtypeStruct((block[2], lanes), f32),
            ),
            in_specs=[pl.BlockSpec(memory_space=pltpu.HBM)],
            out_specs=(vmem, vmem),
            scratch_shapes=[
                pltpu.VMEM((4,) + matrix, f32),
                pltpu.VMEM((2, 4) + matrix, f32),
                pltpu.VMEM((3, 4) + both, f32),
                pltpu.VMEM((len(PAIRS),) + both, f32),
                pltpu.VMEM((2, 4, 8, rows, lanes), f32),
                pltpu.VMEM((2, 3, 4, 8, 2 * rows, lanes), f32),
                pltpu.VMEM((2, len(PAIRS), 8, 2 * rows, lanes), f32),
                pltpu.VMEM((block[2], lanes), f32),
                pltpu.VMEM((sizes[0] * sizes[1], block[2], lanes), f32),
                pltpu.SemaphoreType.DMA((3, count)),
                pltpu.SemaphoreType.DMA((3, count)),
                pltpu.SemaphoreType.DMA((len(partners),)),
                pltpu.SemaphoreType.DMA((len(partners),)),
                pltpu.SemaphoreType.DMA,
            ],
            compiler_params=pltpu.CompilerParams(
                collective_id=0, has_side_effects=True, vmem_limit_bytes=48 * 2**20
            ),
        )(links.reshape((4,) + matrix))
        return flowed.reshape(links.shape), action[:, 0]

    spec = P(None, None, None, None, "gx", "gy", "ta", None)
    return jax.shard_map(
        local, mesh=mesh, in_specs=(spec,), out_specs=(spec, P("ta")), check_vma=False
    )
```
